32 devices in a mesh: gx: 8 (over y, x, core), gy: 4 (over z).
Axes of the slice: x: 2, y: 2, z: 4, core: 2. Of those that a mesh axis runs over, the one named last changes fastest.
Arguments:
- queries: bfloat16 [512, 2048], P(('gx', 'gy')), may hold values from -6 to 6
- probe_dev: int32 [512, 16], P(('gx', 'gy')), may hold values from 0 to 31, all different within a row; in each aligned block of 16 rows (0 to 15, 16 to 31, ...) at most 10 rows name the same one
- probe_list: int32 [512, 16], P(('gx', 'gy')), may hold values from 0 to 15
- documents: bfloat16 [512, 256, 2048], P(('gx', 'gy')), may hold values from -6 to 6
- lengths: int32 [512], P(('gx', 'gy')), may hold values from 96 to 256, as said below
- short_dev: int32 [512, 32], P(('gx', 'gy')), may hold values from 0 to 31, all different within a row; in each aligned block of 16 rows (0 to 15, 16 to 31, ...) at most 16 rows name the same one
- short_list: int32 [512, 32], P(('gx', 'gy')), may hold values from 0 to 15
- short_row: int32 [512, 32], P(('gx', 'gy')), may hold values from 0 to 95
Outputs:
- prefix_top: float32 [512, 32], P(('gx', 'gy'))
- rescored: float32 [512, 32], P(('gx', 'gy'))
The draws below stay inside these ranges and needn't reach their ends.
Inputs may be any that keep to these rules, and one draw needn't show every extreme that they name: `lengths`: every list holds at least 96 documents, and in every draw some list is full. `probe_dev`: the 16 entries of a query name different devices. Among the 16 queries of one device, no device is named more than 10 times, and some device is named exactly 10 times. `short_dev`: the 32 entries of a query name different devices. Among the 16 queries of one device, no device is named more than 16 times, and some device is named exactly 16 times.
All inputs are finite; a program needn't handle non-finite values.
Results may differ from the reference program's by a relative error of at most 0.0029.
Values may be sent and summed in bfloat16 or wider, within the bound.
No kernel may reach another device: no remote copies, remote signals or barrier semaphores. Data moves between devices by JAX's collectives and lax.ppermute only.
A program may use at most 128 MiB of HBM per device.

```python
import math
import jax
import jax.numpy as jnp
import numpy as np
from jax import lax

QRY_DEV = 16
LISTS_DEV = 16
ROWS = 256
LEN_MIN = 96
PREFIX = 256
FULL = 2048
PROBES = 16
TOPK = 32
SHORT = 32
QUERIES = 512
LISTS = 512
CAP = 16
PCAP = 10
DEVICES = 32


def draw_lengths(key, part):
    first_key, second_key = jax.random.split(jax.random.fold_in(key, 17))
    counts = jax.random.randint(first_key, (LISTS,), LEN_MIN, ROWS + 1)
    full_spot = jax.random.randint(second_key, (), 0, LISTS)
    return jnp.where(jnp.arange(LISTS) == full_spot, ROWS, counts).astype(jnp.int32)


def plant(entries, key, smallest, top_value):
    spot = [jax.random.randint(jax.random.fold_in(key, axis), (), 0, length) for axis, length in enumerate(entries.shape)]
    main_axis = entries.shape.index(max(entries.shape))
    neighbour = spot[:main_axis] + [(spot[main_axis] + 1) % entries.shape[main_axis]] + spot[main_axis + 1:]
    return entries.at[tuple(spot)].set(smallest).at[tuple(neighbour)].set(top_value)


def steps_of(rng, extent, cuts, least, largest):
    factor_of, own = 1.0, jax.random.fold_in(rng, 6)
    for position, blocks in cuts:
        steps = jnp.exp(jax.random.uniform(jax.random.fold_in(own, position), (blocks,), jnp.float32, least / len(cuts), largest / len(cuts)))
        factor_of = factor_of * jnp.repeat(steps, extent[position] // blocks).reshape([-1 if axis == position else 1 for axis in range(len(extent))])
    return factor_of


def deal_out(own_key, own, number, rows, number_of, top, reach, skew):
    ranking = jax.random.permutation(own_key, number_of)
    heavy_load, ordinary = load_shares(number_of, rows * top, reach, skew, True), load_shares(number_of, rows * top, reach, skew, False)
    places = jnp.arange(number_of)

    def named(sizes, offset_by):
        used = int((sizes > 0).sum())
        fixed = max(1, used // 4)
        shifted = fixed + (places - fixed + offset_by * (used - fixed)) % max(1, number_of - fixed)
        return jnp.zeros((number_of,), jnp.int32).at[ranking[jnp.where(places < fixed, places, shifted)]].set(jnp.asarray(sizes, jnp.int32))

    sizes = jnp.where(number % 4 == 0, named(heavy_load, number // 4), named(ordinary, number - number // 4 - 1))
    mixed = jax.random.permutation(jax.random.fold_in(own, 3), number_of)
    giver, taker = mixed[0:number_of // 2 * 2:2], mixed[1:number_of // 2 * 2:2]
    margin = jnp.minimum(sizes[giver] - 1, reach - sizes[taker]) // 2
    margin = jnp.where((giver == ranking[0]) | (taker == ranking[0]) | (sizes[taker] == 0), 0, jnp.maximum(margin, 0))
    shifted = jax.random.randint(jax.random.fold_in(own, 4), (number_of // 2,), 0, 1 << 20) % (margin + 1)
    sizes = sizes.at[giver].add(-shifted).at[taker].add(shifted)
    members = jnp.searchsorted(jnp.cumsum(sizes), jnp.arange(rows * top), side="right").astype(jnp.int32)
    table = members.reshape(top, rows).T
    table = table[jax.random.permutation(jax.random.fold_in(own, 1), rows)]
    offset_by = jax.random.randint(jax.random.fold_in(own, 2), (rows, 1), 0, top)
    return jnp.take_along_axis(table, (jnp.arange(top)[None, :] + offset_by) % top, axis=1)


def load_shares(count, total, reach, skew, full):
    portions = [(1 << 20) // math.isqrt(grade ** skew) + 1 for grade in range(1, count + 1)]
    largest = reach if full else min(reach, max(-(-total // count), total * portions[0] // sum(portions)))
    least = 1 if total - largest >= count - 1 else 0
    given, rest = [largest] + [least] * (count - 1), total - largest - least * (count - 1)
    while rest > 0:
        movable = [i for i in range(1, count) if given[i] < largest] or [i for i in range(1, count) if given[i] < reach]
        whole, budget = sum([portions[i] for i in movable]), rest
        for i in movable:
            extra = min(reach - given[i], max(1, budget * portions[i] // whole), rest)
            given[i] = given[i] + extra
            rest = rest - extra
    return np.array(given)


def gaussian(rng, shape, deviation, bound, cuts=(), held_as=jnp.bfloat16):
    result = jax.random.normal(rng, shape, jnp.float32) * deviation
    if len(cuts) > 0:
        result = steps_of(rng, shape, cuts, -0.22, 0.18) * result
    return jnp.clip(result, min=-bound, max=bound).astype(held_as)


def setup_inputs(seed: int = 0) -> dict:
    key_of = jax.random.split(jax.random.key(seed), 9)
    queries = gaussian(key_of[0], (QUERIES, FULL), 1.0, 6.0, ((0, 32),))
    probe_dev_keys = jax.random.split(jax.random.fold_in(key_of[1], 1), QUERIES // QRY_DEV)
    probe_dev_turns = jax.random.permutation(jax.random.fold_in(key_of[1], 3), QUERIES // QRY_DEV)
    probe_dev = jax.vmap(lambda own, number: deal_out(jax.random.fold_in(key_of[1], 2), own, number, QRY_DEV, DEVICES, PROBES, PCAP, 2))(probe_dev_keys, probe_dev_turns).reshape((QUERIES, PROBES))
    probe_list = plant(jax.random.randint(key_of[2], (QUERIES, PROBES), 0, LISTS_DEV), jax.random.fold_in(key_of[2], 1), 0, LISTS_DEV - 1).astype(jnp.int32)
    documents = gaussian(key_of[3], (LISTS, ROWS, FULL), 1.0, 6.0, ((0, 32),))
    lengths = draw_lengths(jax.random.fold_in(key_of[8], 71), 0)
    short_dev_keys = jax.random.split(jax.random.fold_in(key_of[5], 1), QUERIES // QRY_DEV)
    short_dev_turns = jax.random.permutation(jax.random.fold_in(key_of[5], 3), QUERIES // QRY_DEV)
    short_dev = jax.vmap(lambda own, number: deal_out(jax.random.fold_in(key_of[5], 2), own, number, QRY_DEV, DEVICES, SHORT, CAP, 1))(short_dev_keys, short_dev_turns).reshape((QUERIES, SHORT))
    short_list = plant(jax.random.randint(key_of[6], (QUERIES, SHORT), 0, LISTS_DEV), jax.random.fold_in(key_of[6], 1), 0, LISTS_DEV - 1).astype(jnp.int32)
    short_row = plant(jax.random.randint(key_of[7], (QUERIES, SHORT), 0, LEN_MIN), jax.random.fold_in(key_of[7], 1), 0, LEN_MIN - 1).astype(jnp.int32)
    return dict(queries=queries, probe_dev=probe_dev, probe_list=probe_list, documents=documents, lengths=lengths, short_dev=short_dev, short_list=short_list, short_row=short_row)


def unit_rows(values):
    return values / jnp.sqrt(1.0 + lax.optimization_barrier(jnp.sum(values * values, axis=1, keepdims=True)))

def top_values(values, count):
    return -jnp.sort(-values, axis=-1)[..., :count]

def reference(queries, probe_dev, probe_list, documents, lengths, short_dev, short_list, short_row):
    query_float = queries.astype(jnp.float32)
    prefix_unit = unit_rows(query_float[:, :PREFIX]).astype(jnp.bfloat16)
    full_unit = unit_rows(query_float).astype(jnp.bfloat16)
    doc_prefix = documents[:, :, :PREFIX]
    probes = (probe_dev * LISTS_DEV + probe_list).astype(jnp.int32)
    query_total = queries.shape[0]
    block_rows = 64 if query_total % 64 == 0 else query_total

    def top_block(inputs):
        prefix_block, probe_block = inputs
        gathered = doc_prefix[probe_block]
        scores = jnp.einsum('bd,bprd->bpr', prefix_block.astype(jnp.float32), gathered.astype(jnp.float32))
        valid_rows = jnp.arange(ROWS)[None, None, :] < lengths[probe_block][:, :, None]
        masked = jnp.where(valid_rows, scores, -jnp.inf).reshape(prefix_block.shape[0], -1)
        return top_values(masked, TOPK)
    prefix_top = lax.map(top_block, (prefix_unit.reshape(-1, block_rows, PREFIX), probes.reshape(-1, block_rows, PROBES))).reshape(query_total, TOPK)

    def rescore_block(inputs):
        unit_block, dev_block, list_block, row_block = inputs
        list_index = (dev_block * LISTS_DEV + list_block).astype(jnp.int32)
        vectors = documents[list_index, row_block.astype(jnp.int32)]
        return jnp.einsum('bsf,bf->bs', vectors.astype(jnp.float32), unit_block.astype(jnp.float32))
    rescored = lax.map(rescore_block, (full_unit.reshape(-1, block_rows, FULL), short_dev.reshape(-1, block_rows, SHORT), short_list.reshape(-1, block_rows, SHORT), short_row.reshape(-1, block_rows, SHORT))).reshape(query_total, SHORT)
    return (prefix_top, rescored)
```

```python
import jax
import jax.numpy as jnp
from jax import lax
from jax.experimental import pallas as pl
from jax.experimental.pallas import tpu as pltpu
from jax.sharding import PartitionSpec as P

PREFIX = 256
TOPK = 32
AXES = ("gx", "gy")
LANES = 128


def unit_rows(values):
    return values / jnp.sqrt(1.0 + jnp.sum(values * values, axis=1, keepdims=True))


def swap(values, mask, count_dev):
    return lax.ppermute(values, AXES, [(i, i ^ mask) for i in range(count_dev)])


def gather_groups(own, size_x, size_y):
    count_dev = size_x * size_y
    if size_x != 8:
        masks, rows, bit = [0], own, 1
        while bit < count_dev:
            rows = jnp.concatenate([rows, swap(rows, bit, count_dev)], axis=0)
            masks = masks + [m ^ bit for m in masks]
            bit *= 2
        return [(masks, [(0, rows)])]
    core, along_x, along_y = size_y, 2 * size_y, 4 * size_y
    column = jnp.concatenate(
        [own] + [swap(own, m, count_dev) for m in range(1, size_y)], axis=0
    )
    base = list(range(size_y))
    half = own.shape[1] // 2
    from_x = swap(column, along_x, count_dev)
    from_y = swap(column, along_y, count_dev)
    low = swap(from_x[:, :half], along_y, count_dev)
    high = swap(from_y[:, half:], along_x, count_dev)
    groups = [
        (0, [(0, column)]),
        (along_x, [(0, from_x)]),
        (along_y, [(0, from_y)]),
        (along_x ^ along_y, [(0, low), (half, high)]),
    ]
    out = [([m ^ g for m in base], parts) for g, parts in groups]
    for g, parts in groups:
        other = [(c, swap(a, core, count_dev)) for c, a in parts]
        out.append(([m ^ g ^ core for m in base], other))
    return out


def exchange(v, i, j):
    v[i], v[j] = jnp.maximum(v[i], v[j]), jnp.minimum(v[i], v[j])


def sort_down(v):
    n = len(v)
    p = 1
    while p < n:
        k = p
        while k >= 1:
            for j in range(k % p, n - k, 2 * k):
                for i in range(min(k, n - j - k)):
                    if (i + j) // (2 * p) == (i + j + k) // (2 * p):
                        exchange(v, i + j, i + j + k)
            k //= 2
        p *= 2
    return v


def merge_top(a, b):
    n = len(a)
    v = [jnp.maximum(a[i], b[n - 1 - i]) for i in range(n)]
    d = n // 2
    while d >= 1:
        for i in range(n):
            if i & d == 0:
                exchange(v, i, i + d)
        d //= 2
    return v


def prefix_body(len_ref, list_ref, q_ref, d_ref, o_ref, acc):
    step = pl.program_id(0)

    @pl.when(step == 0)
    def _():
        acc[...] = jnp.full(acc.shape, -jnp.inf, jnp.float32)

    scores = lax.dot_general(
        d_ref[0], q_ref[...], (((1,), (1,)), ((), ())), preferred_element_type=jnp.float32
    )
    rows = lax.broadcasted_iota(jnp.int32, scores.shape, 0)
    keep = (rows < len_ref[step]) & (list_ref[...] == step)
    acc[...] = jnp.where(keep, scores, acc[...])

    @pl.when(step == pl.num_programs(0) - 1)
    def _():
        runs = acc.shape[0] // TOPK

        def tile(t, carry):
            lane = pl.ds(pl.multiple_of(t * LANES, LANES), LANES)
            v = sort_down([acc[runs * i : runs * (i + 1), lane] for i in range(TOPK)])
            shift = runs // 2
            while shift >= 1:
                v = merge_top(v, [pltpu.roll(x, shift, 0) for x in v])
                shift //= 2
            for i in range(TOPK):
                o_ref[i : i + 1, lane] = v[i][0:1]
            return carry

        lax.fori_loop(0, acc.shape[1] // LANES, tile, 0)


def prefix_best(lengths, lists, rows, documents):
    count, list_rows = documents.shape[0], documents.shape[1]
    total = rows.shape[0]
    return pl.pallas_call(
        prefix_body,
        grid_spec=pltpu.PrefetchScalarGridSpec(
            num_scalar_prefetch=1,
            grid=(count,),
            in_specs=[
                pl.BlockSpec((1, total), lambda l, n: (0, 0)),
                pl.BlockSpec((total, PREFIX), lambda l, n: (0, 0)),
                pl.BlockSpec((1, list_rows, PREFIX), lambda l, n: (l, 0, 0)),
            ],
            out_specs=pl.BlockSpec((TOPK, total), lambda l, n: (0, 0)),
            scratch_shapes=[pltpu.VMEM((list_rows, total), jnp.float32)],
        ),
        out_shape=jax.ShapeDtypeStruct((TOPK, total), jnp.float32),
        name="prefix_best",
    )(lengths, lists, rows, documents)


def rescore(found, groups):
    layout, arrays, start = [], [], 0
    for masks, parts in groups:
        for first, array in parts:
            layout.append((start, max(first, PREFIX), first))
            arrays.append(array)
        start += parts[0][1].shape[0]
    block = 16

    def body(d_ref, *refs):
        o_ref = refs[-1]
        at = {}
        for (row, low, first), ref in zip(layout, refs):
            at.setdefault(row, []).append((low, first, ref))
        for row, parts in at.items():

            def step(i, carry, row=row, parts=parts):
                here = pl.ds(pl.multiple_of(i * block, block), block)
                there = pl.ds(pl.multiple_of(row + i * block, block), block)
                total = None
                for low, first, ref in parts:
                    for c in range(low, first + ref.shape[1], LANES):
                        q = ref[here, c - first : c - first + LANES].astype(jnp.float32)
                        d = d_ref[there, c - PREFIX : c - PREFIX + LANES].astype(jnp.float32)
                        total = q * d if total is None else total + q * d
                o_ref[there, :] = jnp.sum(total, axis=1, keepdims=True)
                return carry

            lax.fori_loop(0, parts[0][2].shape[0] // block, step, 0, unroll=2)

    vmem = pl.BlockSpec(memory_space=pltpu.VMEM)
    return pl.pallas_call(
        body,
        in_specs=[vmem] * (1 + len(arrays)),
        out_specs=vmem,
        out_shape=jax.ShapeDtypeStruct((found.shape[0], 1), jnp.float32),
        name="rescore",
    )(found, *arrays)


def merge_best(runs, queries):
    def body(x_ref, o_ref):
        v = [x_ref[i] for i in range(TOPK)]
        size = x_ref.shape[1]
        while size > 1:
            size //= 2
            v = merge_top([x[:size] for x in v], [x[size : 2 * size] for x in v])
        shift = LANES // 2
        while shift >= queries:
            v = merge_top(v, [pltpu.roll(x, shift, 1) for x in v])
            shift //= 2
        for i in range(TOPK):
            o_ref[i : i + 1, :] = v[i]

    return pl.pallas_call(
        body,
        out_shape=jax.ShapeDtypeStruct((TOPK, LANES), jnp.float32),
        name="merge_best",
    )(runs)


def shards(queries, probe_dev, probe_list, documents, lengths, short_dev, short_list, short_row):
    size_x, size_y = lax.axis_size("gx"), lax.axis_size("gy")
    count_dev = size_x * size_y
    me = lax.axis_index(AXES)
    query_rows = queries.shape[0]
    rows_list = documents.shape[1]
    devices = jnp.arange(count_dev, dtype=jnp.int32)[:, None, None]

    probe_code = jnp.sum(jnp.where(probe_dev[None] == devices, probe_list[None] + 1, 0), axis=2)
    wanted = short_list * rows_list + short_row
    short_code = jnp.sum(jnp.where(short_dev[None] == devices, wanted[None] + 1, 0), axis=2)
    codes = jnp.concatenate([probe_code, short_code], axis=1)
    got = lax.all_to_all(codes, AXES, split_axis=0, concat_axis=0, tiled=True)

    query_float = queries.astype(jnp.float32)
    prefix_unit = unit_rows(query_float[:, :PREFIX]).astype(jnp.bfloat16)
    full_unit = unit_rows(query_float).astype(jnp.bfloat16)
    own = jnp.concatenate([prefix_unit, full_unit], axis=1)
    groups = gather_groups(own, size_x, size_y)
    masks = [m for group, _ in groups for m in group]
    slot_of = [masks.index(m) for m in range(count_dev)]

    got = got[jnp.array(masks, jnp.int32) ^ me]
    lists = got[:, :query_rows].reshape(1, -1) - 1
    picks = jnp.maximum(got[:, query_rows:].reshape(-1) - 1, 0)
    found = documents.reshape(-1, documents.shape[2])[picks]

    prefixes = jnp.concatenate([parts[0][1][:, :PREFIX] for _, parts in groups], axis=0)
    best = prefix_best(lengths, lists, prefixes, documents)
    scored = rescore(found, groups)

    best = best.reshape(TOPK, count_dev, query_rows).transpose(1, 0, 2)
    scored = scored.reshape(count_dev, 1, query_rows)
    results = jnp.concatenate([best, scored], axis=1).reshape(count_dev, -1)
    results = results[jnp.array(slot_of, jnp.int32)[jnp.arange(count_dev) ^ me]]
    back = lax.all_to_all(results, AXES, split_axis=0, concat_axis=0, tiled=True)
    back = back.reshape(count_dev, TOPK + 1, query_rows)

    runs = back[:, :TOPK].transpose(1, 0, 2).reshape(TOPK, -1, LANES)
    prefix_top = merge_best(runs, query_rows)[:, :query_rows].T
    answers = back[:, TOPK].T[:, None, :]
    hits = short_dev[:, :, None] == jnp.arange(count_dev, dtype=jnp.int32)[None, None, :]
    rescored = jnp.sum(jnp.where(hits, answers, 0.0), axis=2)
    return (prefix_top, rescored)


def solution(mesh):
    in_specs = (
        P(AXES, None),
        P(AXES, None),
        P(AXES, None),
        P(AXES, None, None),
        P(AXES),
        P(AXES, None),
        P(AXES, None),
        P(AXES, None),
    )
    out_specs = (P(AXES, None), P(AXES, None))
    return jax.shard_map(shards, mesh=mesh, in_specs=in_specs, out_specs=out_specs, check_vma=False)
```

```python
import jax
import jax.numpy as jnp
from jax import lax
from jax.experimental import pallas as pl
from jax.experimental.pallas import tpu as pltpu
from jax.sharding import PartitionSpec as P

PREFIX = 256
TOPK = 32
AXES = ("gx", "gy")
LANES = 128


def unit_rows(values):
    return values / jnp.sqrt(1.0 + jnp.sum(values * values, axis=1, keepdims=True))


def swap(values, mask, count_dev):
    return lax.ppermute(values, AXES, [(i, i ^ mask) for i in range(count_dev)])


def send_codes(codes, masks, me):
    got = lax.all_to_all(codes, AXES, split_axis=0, concat_axis=0, tiled=True)
    return got[jnp.array(masks, jnp.int32) ^ me]


def gather_groups(own, codes, me, size_x, size_y):
    count_dev = size_x * size_y
    if size_x != 8:
        masks, rows, bit = [0], own, 1
        while bit < count_dev:
            rows = jnp.concatenate([rows, swap(rows, bit, count_dev)], axis=0)
            masks = masks + [m ^ bit for m in masks]
            bit *= 2
        return [[(masks, [(0, rows)])]], [send_codes(codes, masks, me)]
    core, along_x, along_y = size_y, 2 * size_y, 4 * size_y
    column = jnp.concatenate(
        [own] + [swap(own, m, count_dev) for m in range(1, size_y)], axis=0
    )
    codes, column = lax.optimization_barrier((codes, column))
    half = own.shape[1] // 2
    heads = [g ^ c for c in (0, core) for g in (0, along_x, along_y, along_x ^ along_y)]
    masks = [h ^ m for h in heads for m in range(size_y)]
    from_x = swap(column, along_x, count_dev)
    from_y = swap(column, along_y, count_dev)
    got = send_codes(codes, masks, me)
    got, from_x, from_y = lax.optimization_barrier((got, from_x, from_y))
    middle = got.shape[0] // 2
    first, second = got[:middle], got[middle:]
    low = swap(from_x[:, :half], along_y, count_dev)
    high = swap(from_y[:, half:], along_x, count_dev)
    second, low, high = lax.optimization_barrier((second, low, high))
    parts = [[(0, column)], [(0, from_x)], [(0, from_y)], [(0, low), (half, high)]]
    other = [[(c, swap(rows, core, count_dev)) for c, rows in part] for part in parts]
    groups = [
        (masks[i * size_y : (i + 1) * size_y], part) for i, part in enumerate(parts + other)
    ]
    return [groups[:4], groups[4:]], [first, second]


def unit_body(q_ref, o_ref):
    values = q_ref[...].astype(jnp.float32)
    o_ref[:, :PREFIX] = unit_rows(values[:, :PREFIX]).astype(jnp.bfloat16)
    o_ref[:, PREFIX:] = unit_rows(values).astype(jnp.bfloat16)


def unit_pair(queries):
    rows, width = queries.shape
    return pl.pallas_call(
        unit_body,
        out_shape=jax.ShapeDtypeStruct((rows, PREFIX + width), jnp.bfloat16),
        name="unit_pair",
    )(queries)


def exchange(v, i, j):
    v[i], v[j] = jnp.maximum(v[i], v[j]), jnp.minimum(v[i], v[j])


def sort_down(v):
    n = len(v)
    p = 1
    while p < n:
        k = p
        while k >= 1:
            for j in range(k % p, n - k, 2 * k):
                for i in range(min(k, n - j - k)):
                    if (i + j) // (2 * p) == (i + j + k) // (2 * p):
                        exchange(v, i + j, i + j + k)
            k //= 2
        p *= 2
    return v


def merge_top(a, b):
    n = len(a)
    v = [jnp.maximum(a[i], b[n - 1 - i]) for i in range(n)]
    d = n // 2
    while d >= 1:
        for i in range(n):
            if i & d == 0:
                exchange(v, i, i + d)
        d //= 2
    return v


def prefix_body(len_ref, list_ref, q_ref, d_ref, o_ref, acc):
    step = pl.program_id(0)
    each = d_ref.shape[0]
    lists = list_ref[...]
    best = acc[...]
    for i in range(each):
        scores = lax.dot_general(
            d_ref[i], q_ref[...], (((1,), (1,)), ((), ())), preferred_element_type=jnp.float32
        )
        best = jnp.where(lists == step * each + i, scores, best)
    acc[...] = best

    @pl.when(step == pl.num_programs(0) - 1)
    def _():
        runs = acc.shape[0] // TOPK

        def tile(t, carry):
            lane = pl.ds(pl.multiple_of(t * LANES, LANES), LANES)
            own = list_ref[:, lane]
            held = jnp.zeros_like(own)
            for l in range(len_ref.shape[0]):
                held = jnp.where(own == l, len_ref[l], held)
            rows = lax.broadcasted_iota(jnp.int32, (runs, LANES), 0)
            v = [
                jnp.where(rows + runs * i < held, acc[runs * i : runs * (i + 1), lane], -jnp.inf)
                for i in range(TOPK)
            ]
            v = sort_down(v)
            shift = runs // 2
            while shift >= 1:
                v = merge_top(v, [pltpu.roll(x, shift, 0) for x in v])
                shift //= 2
            for i in range(TOPK):
                o_ref[i : i + 1, lane] = v[i][0:1]
            return carry

        lax.fori_loop(0, acc.shape[1] // LANES, tile, 0)


def prefix_best(lengths, lists, rows, documents):
    count, list_rows = documents.shape[0], documents.shape[1]
    total = rows.shape[0]
    each = 4 if count % 4 == 0 else 1
    return pl.pallas_call(
        prefix_body,
        grid_spec=pltpu.PrefetchScalarGridSpec(
            num_scalar_prefetch=1,
            grid=(count // each,),
            in_specs=[
                pl.BlockSpec((1, total), lambda l, n: (0, 0)),
                pl.BlockSpec((total, PREFIX), lambda l, n: (0, 0)),
                pl.BlockSpec((each, list_rows, PREFIX), lambda l, n: (l, 0, 0)),
            ],
            out_specs=pl.BlockSpec((TOPK, total), lambda l, n: (0, 0)),
            scratch_shapes=[pltpu.VMEM((list_rows, total), jnp.float32)],
        ),
        out_shape=jax.ShapeDtypeStruct((TOPK, total), jnp.float32),
        name="prefix_best",
    )(lengths, lists, rows, documents)


def rescore(found, groups):
    layout, arrays, start = [], [], 0
    for masks, parts in groups:
        for first, array in parts:
            layout.append((start, max(first, PREFIX), first))
            arrays.append(array)
        start += parts[0][1].shape[0]
    block = 16

    def body(d_ref, *refs):
        o_ref = refs[-1]
        at = {}
        for (row, low, first), ref in zip(layout, refs):
            at.setdefault(row, []).append((low, first, ref))
        for row, parts in at.items():

            def step(i, carry, row=row, parts=parts):
                here = pl.ds(pl.multiple_of(i * block, block), block)
                there = pl.ds(pl.multiple_of(row + i * block, block), block)
                total = None
                for low, first, ref in parts:
                    for c in range(low, first + ref.shape[1], LANES):
                        q = ref[here, c - first : c - first + LANES].astype(jnp.float32)
                        d = d_ref[there, c - PREFIX : c - PREFIX + LANES].astype(jnp.float32)
                        total = q * d if total is None else total + q * d
                o_ref[there, :] = jnp.sum(total, axis=1, keepdims=True)
                return carry

            lax.fori_loop(0, parts[0][2].shape[0] // block, step, 0, unroll=2)

    vmem = pl.BlockSpec(memory_space=pltpu.VMEM)
    return pl.pallas_call(
        body,
        in_specs=[vmem] * (1 + len(arrays)),
        out_specs=vmem,
        out_shape=jax.ShapeDtypeStruct((found.shape[0], 1), jnp.float32),
        name="rescore",
    )(found, *arrays)


def merge_best(runs, queries):
    def body(x_ref, o_ref):
        v = [x_ref[i] for i in range(TOPK)]
        size = x_ref.shape[1]
        while size > 1:
            size //= 2
            v = merge_top([x[:size] for x in v], [x[size : 2 * size] for x in v])
        shift = LANES // 2
        while shift >= queries:
            v = merge_top(v, [pltpu.roll(x, shift, 1) for x in v])
            shift //= 2
        for i in range(TOPK):
            o_ref[i : i + 1, :] = v[i]

    return pl.pallas_call(
        body,
        out_shape=jax.ShapeDtypeStruct((TOPK, LANES), jnp.float32),
        name="merge_best",
    )(runs)


def shards(queries, probe_dev, probe_list, documents, lengths, short_dev, short_list, short_row):
    size_x, size_y = lax.axis_size("gx"), lax.axis_size("gy")
    count_dev = size_x * size_y
    me = lax.axis_index(AXES)
    query_rows = queries.shape[0]
    rows_list = documents.shape[1]
    devices = jnp.arange(count_dev, dtype=jnp.int32)[:, None, None]

    probe_code = jnp.sum(jnp.where(probe_dev[None] == devices, probe_list[None] + 1, 0), axis=2)
    wanted = short_list * rows_list + short_row
    short_code = jnp.sum(jnp.where(short_dev[None] == devices, wanted[None] + 1, 0), axis=2)
    codes = jnp.concatenate([probe_code, short_code], axis=1)

    own = unit_pair(queries)
    sides, tables = gather_groups(own, codes, me, size_x, size_y)
    groups = [group for side in sides for group in side]
    masks = [m for group, _ in groups for m in group]
    slot_of = [masks.index(m) for m in range(count_dev)]

    doc_table = documents.reshape(-1, documents.shape[2])
    scored = []
    for side, table in zip(sides, tables):
        picks = jnp.maximum(table[:, query_rows:].reshape(-1) - 1, 0)
        scored.append(rescore(doc_table[picks], side))
    scored = jnp.concatenate(scored, axis=0)
    lists = jnp.concatenate(tables, axis=0)[:, :query_rows].reshape(1, -1) - 1
    prefixes = jnp.concatenate([parts[0][1][:, :PREFIX] for _, parts in groups], axis=0)
    best = prefix_best(lengths, lists, prefixes, documents)

    best = best.reshape(TOPK, count_dev, query_rows).transpose(1, 0, 2)
    scored = scored.reshape(count_dev, 1, query_rows)
    results = jnp.concatenate([best, scored], axis=1).reshape(count_dev, -1)
    results = results[jnp.array(slot_of, jnp.int32)[jnp.arange(count_dev) ^ me]]
    back = lax.all_to_all(results, AXES, split_axis=0, concat_axis=0, tiled=True)
    back = back.reshape(count_dev, TOPK + 1, query_rows)

    runs = back[:, :TOPK].transpose(1, 0, 2).reshape(TOPK, -1, LANES)
    prefix_top = merge_best(runs, query_rows)[:, :query_rows].T
    answers = back[:, TOPK].T[:, None, :]
    hits = short_dev[:, :, None] == jnp.arange(count_dev, dtype=jnp.int32)[None, None, :]
    rescored = jnp.sum(jnp.where(hits, answers, 0.0), axis=2)
    return (prefix_top, rescored)


def solution(mesh):
    in_specs = (
        P(AXES, None),
        P(AXES, None),
        P(AXES, None),
        P(AXES, None, None),
        P(AXES),
        P(AXES, None),
        P(AXES, None),
        P(AXES, None),
    )
    out_specs = (P(AXES, None), P(AXES, None))
    return jax.shard_map(shards, mesh=mesh, in_specs=in_specs, out_specs=out_specs, check_vma=False)
```
